256 devices in a mesh: mat: 4 (over z_lo), tile: 64 (over y, z_hi, x, core).
Axes of the slice: x: 4, y: 4, z: 8 (z_hi: 2, z_lo: 4; z = z_hi * 4 + z_lo), core: 2. Of those that a mesh axis runs over, the one named last changes fastest.
Arguments:
- volume: bfloat16 [4, 512, 64, 1024], P('mat', None, 'tile'), may hold values from -4 to 4
- system: bfloat16 [64, 1024, 32, 128], P('tile'), may hold values from 0 to 0.009521484
- geometry: int32 [64, 16], replicated, may hold values from 0 to 2
- attenuation: float32 [4, 64], replicated, may hold values from 0.05 to 0.5
- response: float32 [8, 64], replicated, may hold values from 0.002 to 0.06
- crosstalk: float32 [8], replicated, may hold values from 0.04 to 0.24
Outputs:
- counts: float32 [8, 512, 16, 512], P(None, ('mat', 'tile'))
The draws below stay inside these ranges and needn't reach their ends.
Inputs may be any that keep to these rules, and one draw needn't show every extreme that they name: A tile touches, in view v, exactly the 2 detector blocks geometry[t, v] to geometry[t, v] + 1.
All inputs are finite; a program needn't handle non-finite values.
Results may differ from the reference program's by a relative error of at most 0.0003.
Values may be sent and summed in bfloat16 or wider, within the bound.
No kernel may reach another device: no remote copies, remote signals or barrier semaphores. Data moves between devices by JAX's collectives and lax.ppermute only.
A program may use at most 128 MiB of HBM per device.

```python
import math
import jax
import jax.numpy as jnp
from jax import lax

MATS = 4
TILE_VOX = 1024
VIEWS = 16
PIXELS = 512
PB = 128
TOUCH = 2
EBINS = 64
CBINS = 8
TILES = 64
SLICES = 512
PBLK = 4
KT = 32
RAYS = 8192


def place_ends(entries, rng, least, largest):
    shape = entries.shape
    place = [jax.random.randint(jax.random.fold_in(rng, axis), (), 0, shape[axis]) for axis in range(len(shape))]
    entries = entries.at[tuple(place)].set(least)
    longest = shape.index(max(shape))
    place[longest] = (place[longest] + 1) % shape[longest]
    return entries.at[tuple(place)].set(largest)


def level_of(stream_key, shape, cuts, low, high):
    level = 1.0
    for dim, shards_of in cuts:
        steps = jax.random.uniform(jax.random.fold_in(jax.random.fold_in(stream_key, 6), dim), (shards_of,), jnp.float32, low / len(cuts), high / len(cuts))
        level = level * jnp.repeat(jnp.exp(steps), shape[dim] // shards_of).reshape((-1,) + (1,) * (len(shape) - 1 - dim))
    return level


def noise(own_key, extent, width, bound, split=(), kind=jnp.bfloat16):
    values = jax.random.normal(own_key, extent, jnp.float32) * width
    if len(split) > 0:
        values = level_of(own_key, extent, split, -0.22, 0.18) * values
    return jnp.clip(values, min=-bound, max=bound).astype(kind)


def setup_inputs(seed: int = 0) -> dict:
    arg_keys = jax.random.split(jax.random.key(seed), 7)
    volume = noise(arg_keys[0], (MATS, SLICES, TILES, TILE_VOX), 1.0, 4.0, ((0, 4), (2, 64)))
    system = jnp.clip(0.009521484 * jax.random.uniform(arg_keys[1], (TILES, TILE_VOX, KT, PB), jnp.float32) ** level_of(arg_keys[1], (TILES, TILE_VOX, KT, PB), ((0, 64),), -0.2, 0.2), 0.0, 0.009521484).astype(jnp.bfloat16)
    geometry = place_ends(jax.random.randint(arg_keys[2], (TILES, VIEWS), 0, PBLK - TOUCH + 1), jax.random.fold_in(arg_keys[2], 1), 0, PBLK - TOUCH).astype(jnp.int32)
    attenuation = jnp.clip(jnp.exp(jax.random.uniform(arg_keys[3], (MATS, EBINS), jnp.float32, math.log(0.05), math.log(0.5))), 0.05, 0.5)
    response = jnp.clip(jnp.exp(jax.random.uniform(arg_keys[4], (CBINS, EBINS), jnp.float32, math.log(0.002), math.log(0.06))), 0.002, 0.06)
    crosstalk = jnp.clip(jax.random.uniform(arg_keys[5], (CBINS,), jnp.float32, 0.04, 0.24), 0.04, 0.24)
    return {"volume": volume, "system": system, "geometry": geometry, "attenuation": attenuation, "response": response, "crosstalk": crosstalk}


def reference(volume, system, geometry, attenuation, response, crosstalk):
    row_total = MATS * SLICES
    block_ids = jnp.arange(PBLK, dtype=jnp.int32)
    touch_ids = jnp.arange(TOUCH, dtype=jnp.int32)

    def one_tile(running, tile_index):
        columns = lax.dynamic_index_in_dim(volume, tile_index, 2, keepdims=False)
        columns = columns.reshape(row_total, TILE_VOX).astype(jnp.float32)
        matrix = lax.dynamic_index_in_dim(system, tile_index, 0, keepdims=False)
        matrix = matrix.reshape(TILE_VOX, KT * PB).astype(jnp.float32)
        partial_value = jnp.dot(columns, matrix, preferred_element_type=jnp.float32, precision=lax.Precision.HIGHEST)
        partial_value = partial_value.reshape(row_total, VIEWS, TOUCH, PB)
        first_block = lax.dynamic_index_in_dim(geometry, tile_index, 0, keepdims=False)
        placed = (first_block[:, None, None] + touch_ids[None, :, None] == block_ids[None, None, :]).astype(jnp.float32)
        expanded = jnp.einsum('rvjp,vjb->rvbp', partial_value, placed, precision=lax.Precision.HIGHEST)
        return (running + expanded, None)
    start_sums = jnp.zeros((row_total, VIEWS, PBLK, PB), jnp.float32)
    summed = lax.scan(one_tile, start_sums, jnp.arange(TILES, dtype=jnp.int32))[0]
    proj = summed.reshape(MATS, SLICES, RAYS).transpose(1, 0, 2)

    def one_row(integrals):
        exponent = jnp.dot(attenuation.T, integrals, preferred_element_type=jnp.float32, precision=lax.Precision.HIGHEST)
        return jnp.dot(response, jnp.exp(-exponent), preferred_element_type=jnp.float32, precision=lax.Precision.HIGHEST)
    detected = lax.map(one_row, proj).transpose(1, 0, 2)
    padded = jnp.pad(detected, ((0, 0), (1, 1), (0, 0)))
    leakage = crosstalk[:, None, None]
    counts = (1.0 - 2.0 * leakage) * detected + leakage * (padded[:, :-2] + padded[:, 2:])
    return counts.reshape(CBINS, SLICES, VIEWS, PIXELS)
```

```python
import functools

import jax
import jax.numpy as jnp
from jax import lax
from jax.experimental import pallas as pl
from jax.experimental.pallas import tpu as pltpu
from jax.sharding import Mesh, PartitionSpec as P

PB = 128
PBLK = 4
CBINS = 8
EBINS = 64
MATS = 4
AXES = ("mat", "y", "zh", "x", "core")
TILE_AXES = ("y", "zh", "x", "core")
PAIRS = ([(0, 1), (1, 0), (2, 3), (3, 2)], [(1, 2), (2, 1), (3, 0), (0, 3)])
ORDERS = (
    (("x", 0), ("y", 0), ("x", 1), ("y", 1)),
    (("x", 1), ("y", 1), ("x", 0), ("y", 0)),
    (("y", 0), ("x", 0), ("y", 1), ("x", 1)),
    (("y", 1), ("x", 1), ("y", 0), ("x", 0)),
)
DIM_OF = {("x", 0): 2, ("x", 1): 3, ("y", 0): 4, ("y", 1): 5}


def pair_bits(i):
    return ((i + 1) // 2) % 2, i // 2


def row_order(slice_count):
    pos = jnp.arange(slice_count, dtype=jnp.int32)
    bits = [(pos // (256 >> n)) % 2 for n in range(5)]
    rest = pos % 16
    core = bits[0] ^ lax.axis_index("core")

    def place(b0, b1, name):
        mine = pair_bits(lax.axis_index(name))
        b0, b1 = b0 ^ mine[0], b1 ^ mine[1]
        return 2 * b1 + (b0 ^ b1)

    x = place(bits[1], bits[2], "x")
    y = place(bits[3], bits[4], "y")
    mat, zh, r = rest // 4, (rest // 2) % 2, rest % 2
    return mat * 128 + y * 32 + zh * 16 + x * 4 + core * 2 + r


def project_body(vol_ref, sys_ref, out_ref):
    @pl.when(pl.program_id(0) == 0)
    def _():
        out_ref[...] = jnp.zeros_like(out_ref)

    weights = jnp.swapaxes(sys_ref[...], 0, 1)
    for k in range(0, 8, 2):
        pair = jnp.concatenate([weights[k], weights[k + 1]], axis=1)
        got = jnp.dot(vol_ref[...], pair, preferred_element_type=jnp.float32)
        out_ref[k] += got[:, :PB]
        out_ref[k + 1] += got[:, PB:]


def project(columns, matrix, portion):
    rows, depth = columns.shape
    step = 256
    return pl.pallas_call(
        project_body,
        grid=(depth // step,),
        in_specs=[
            pl.BlockSpec((rows, step), lambda i: (0, i)),
            pl.BlockSpec((step, 8, PB), lambda i: (i, portion, 0)),
        ],
        out_specs=pl.BlockSpec((8, rows, PB), lambda i: (0, 0, 0)),
        out_shape=jax.ShapeDtypeStruct((8, rows, PB), jnp.float32),
        name="project",
    )(columns, matrix)


def placed(pieces, first):
    shape = (4, PBLK) + (1,) * (pieces.ndim - 2)
    offset = jnp.arange(PBLK, dtype=jnp.int32)[None, :] - first[:, None]
    offset = offset.reshape(shape)
    zero = jnp.float32(0)
    low, high = pieces[:, 0:1].astype(jnp.float32), pieces[:, 1:2].astype(jnp.float32)
    return jnp.where(offset == 0, low, jnp.where(offset == 1, high, zero))


def per_device(volume, system, geometry, attenuation, response, crosstalk):
    rows = volume.shape[1]
    depth = volume.shape[3]
    tile = lax.axis_index(TILE_AXES)
    vol = volume.reshape(rows, depth)
    order = row_order(rows)
    chosen = (order[:, None] == jnp.arange(rows, dtype=jnp.int32)[None, :]).astype(jnp.bfloat16)
    columns = jnp.dot(chosen, vol, preferred_element_type=jnp.float32).astype(jnp.bfloat16)
    matrix = system.reshape(depth, 32, PB)
    mine = lax.dynamic_index_in_dim(geometry, tile, 0, keepdims=False)
    partner = lax.dynamic_index_in_dim(geometry, tile ^ 1, 0, keepdims=False)

    current = []
    for w in range(4):
        part = project(columns, matrix, w).reshape(4, 2, 2, 2, 2, 2, 2, 16, PB)
        sent = part[:, :, 1].astype(jnp.float16)
        got = lax.ppermute(sent, "core", [(0, 1), (1, 0)])
        first, other = mine[4 * w : 4 * w + 4], partner[4 * w : 4 * w + 4]
        current.append(placed(part[:, :, 0], first) + placed(got, other))
    for n in range(4):
        for w in range(4):
            step = ORDERS[w][n]
            dim = DIM_OF[step]
            keep = lax.slice_in_dim(current[w], 0, 1, axis=dim)
            sent = lax.slice_in_dim(current[w], 1, 2, axis=dim).astype(jnp.float16)
            got = lax.ppermute(sent, step[0], PAIRS[step[1]])
            current[w] = keep + got.astype(jnp.float32)

    whole = jnp.concatenate([c.reshape(4, PBLK, MATS, 2, 2, PB) for c in current], axis=0)
    outgoing = whole.transpose(3, 2, 4, 0, 1, 5).astype(jnp.float16).reshape(8, 2, 64, PB)
    received = lax.all_to_all(outgoing, ("zh", "mat"), 0, 0, tiled=True)
    received = received.reshape(2, MATS, 2 * 64 * PB).astype(jnp.float32)
    stacked = received[0] + received[1]
    exponent = jnp.dot(attenuation.T, stacked, preferred_element_type=jnp.float32, precision=lax.Precision.HIGHEST)
    detected = jnp.dot(
        response, jnp.exp(-exponent), preferred_element_type=jnp.float32, precision=lax.Precision.HIGHEST
    )
    detected = detected.reshape(CBINS, 2, 64 * PB)
    axes = ("mat",) + TILE_AXES
    count = lax.axis_size(axes)
    up = [(i, i + 1) for i in range(count - 1)]
    above = lax.ppermute(detected[:, 1:], axes, up)
    below = lax.ppermute(detected[:, :1], axes, [(b, a) for a, b in up])
    padded = jnp.concatenate([above, detected, below], axis=1)
    leakage = crosstalk[:, None, None]
    counts = (1.0 - 2.0 * leakage) * detected + leakage * (padded[:, :-2] + padded[:, 2:])
    return counts.reshape(CBINS, 2, 16, PBLK * PB)


def solution(mesh):
    fine = Mesh(mesh.devices.reshape(4, 4, 2, 4, 2), AXES)
    in_specs = (P("mat", None, TILE_AXES, None), P(TILE_AXES, None, None, None), P(), P(), P(), P())
    out_specs = P(None, AXES, None, None)
    return jax.shard_map(per_device, mesh=fine, in_specs=in_specs, out_specs=out_specs, check_vma=False)
```

```python
import functools

import jax
import jax.numpy as jnp
from jax import lax
from jax.experimental import pallas as pl
from jax.experimental.pallas import tpu as pltpu
from jax.sharding import Mesh, PartitionSpec as P

PB = 128
PBLK = 4
CBINS = 8
EBINS = 64
MATS = 4
AXES = ("mat", "y", "zh", "x", "core")
TILE_AXES = ("y", "zh", "x", "core")
PAIRS = ([(0, 1), (1, 0), (2, 3), (3, 2)], [(1, 2), (2, 1), (3, 0), (0, 3)])
ORDERS = (
    (("x", 0), ("y", 0), ("x", 1), ("y", 1)),
    (("x", 1), ("y", 1), ("x", 0), ("y", 0)),
    (("y", 0), ("x", 0), ("y", 1), ("x", 1)),
    (("y", 1), ("x", 1), ("y", 0), ("x", 0)),
)
DIM_OF = {("x", 0): 2, ("x", 1): 3, ("y", 0): 4, ("y", 1): 5}


def pair_bits(i):
    return ((i + 1) // 2) % 2, i // 2


def row_order(slice_count):
    pos = jnp.arange(slice_count, dtype=jnp.int32)
    bits = [(pos // (256 >> n)) % 2 for n in range(5)]
    rest = pos % 16
    core = bits[0] ^ lax.axis_index("core")

    def place(b0, b1, name):
        mine = pair_bits(lax.axis_index(name))
        b0, b1 = b0 ^ mine[0], b1 ^ mine[1]
        return 2 * b1 + (b0 ^ b1)

    x = place(bits[1], bits[2], "x")
    y = place(bits[3], bits[4], "y")
    mat, zh, r = rest // 4, (rest // 2) % 2, rest % 2
    return mat * 128 + y * 32 + zh * 16 + x * 4 + core * 2 + r


def vmem_params(mib):
    return pltpu.CompilerParams(vmem_limit_bytes=mib << 20)


VMEM = pl.BlockSpec(memory_space=pltpu.VMEM)
SMEM = pl.BlockSpec(memory_space=pltpu.SMEM)
HBM = pl.BlockSpec(memory_space=pltpu.HBM)


def multiply(columns, matrix_ref, own_hbm, away_hbm, buf, sems):
    weights = jnp.swapaxes(matrix_ref[...], 0, 1)
    half = columns.shape[0] // 2
    copies = []
    for v in range(4):
        pair = jnp.concatenate([weights[2 * v], weights[2 * v + 1]], axis=1)
        got = jnp.dot(columns, pair, preferred_element_type=jnp.float32)
        buf[v, 0] = got[:, :PB]
        buf[v, 1] = got[:, PB:]
        copies.append(pltpu.make_async_copy(buf.at[v, :, pl.ds(half, half), :], away_hbm.at[v], sems.at[2 * v]))
        copies.append(pltpu.make_async_copy(buf.at[v, :, pl.ds(0, half), :], own_hbm.at[v], sems.at[2 * v + 1]))
        copies[-2].start()
        copies[-1].start()
    return copies


def wait_all(copies):
    for copy in copies:
        copy.wait()


def first_body(
    order_ref, vol_hbm, sys_hbm, own_hbm, away_hbm, col_ref, m1_ref, m2_ref, m3_ref, vol_buf, m0_buf, buf, sems, out_sems
):
    copies = [pltpu.make_async_copy(vol_hbm, vol_buf, sems.at[4])]
    for w, target in enumerate((m0_buf, m1_ref, m2_ref, m3_ref)):
        copies.append(pltpu.make_async_copy(sys_hbm.at[:, pl.ds(8 * w, 8), :], target, sems.at[w]))
    for copy in copies:
        copy.start()
    rows = vol_buf.shape[0]
    chosen = (order_ref[...] == lax.broadcasted_iota(jnp.int32, (rows, rows), 1)).astype(jnp.bfloat16)
    copies[0].wait()
    columns = jnp.dot(chosen, vol_buf[...], preferred_element_type=jnp.float32).astype(jnp.bfloat16)
    col_ref[...] = columns
    copies[1].wait()
    outs = multiply(columns, m0_buf, own_hbm, away_hbm, buf, out_sems)
    wait_all(copies[2:])
    wait_all(outs)


def in_hbm(x):
    return pltpu.with_memory_space_constraint(x, pltpu.HBM)


def project_first(order, vol, matrix):
    rows, depth = vol.shape
    half = pltpu.HBM((4, 2, rows // 2, PB), jnp.float32)
    part = pltpu.VMEM((depth, 8, PB), jnp.bfloat16)
    return pl.pallas_call(
        first_body,
        in_specs=[VMEM, HBM, HBM],
        out_specs=[HBM] * 2 + [VMEM] * 4,
        out_shape=[half, half, pltpu.VMEM((rows, depth), jnp.bfloat16), part, part, part],
        scratch_shapes=[
            pltpu.VMEM((rows, depth), jnp.bfloat16),
            pltpu.VMEM((depth, 8, PB), jnp.bfloat16),
            pltpu.VMEM((4, 2, rows, PB), jnp.float32),
            pltpu.SemaphoreType.DMA((5,)),
            pltpu.SemaphoreType.DMA((8,)),
        ],
        cost_estimate=pl.CostEstimate(flops=2 * rows * depth * 12 * PB, transcendentals=0, bytes_accessed=12 << 20),
        compiler_params=vmem_params(16),
        name="project_first",
    )(order, in_hbm(vol), in_hbm(matrix))


def project_body(col_ref, matrix_ref, own_hbm, away_hbm, buf, out_sems):
    wait_all(multiply(col_ref[...], matrix_ref, own_hbm, away_hbm, buf, out_sems))


def project(columns, matrix):
    rows, depth = columns.shape
    half = pltpu.HBM((4, 2, rows // 2, PB), jnp.float32)
    return pl.pallas_call(
        project_body,
        in_specs=[VMEM, VMEM],
        out_specs=[HBM, HBM],
        out_shape=[half, half],
        scratch_shapes=[pltpu.VMEM((4, 2, rows, PB), jnp.float32), pltpu.SemaphoreType.DMA((8,))],
        cost_estimate=pl.CostEstimate(flops=2 * rows * depth * 8 * PB, transcendentals=0, bytes_accessed=5 << 20),
        compiler_params=vmem_params(10),
        name="project",
    )(columns, matrix)


def merge_body(first_ref, other_ref, own_any, got_any, out_ref, own_buf, got_buf, sems, *, portion, side):
    copies = []
    for v in range(4):
        copies.append(pltpu.make_async_copy(own_any.at[v, :, :, side], own_buf.at[v], sems.at[2 * v]))
        copies.append(pltpu.make_async_copy(got_any.at[v, :, :, side], got_buf.at[v], sems.at[2 * v + 1]))
    for copy in copies:
        copy.start()
    for v in range(4):
        wait_all(copies[2 * v : 2 * v + 2])
        first, other = first_ref[4 * portion + v], other_ref[4 * portion + v]
        for b in range(PBLK):
            mine = jnp.where(first == b, own_buf[v, 0], jnp.where(first + 1 == b, own_buf[v, 1], 0.0))
            theirs = jnp.where(other == b, got_buf[v, 0], jnp.where(other + 1 == b, got_buf[v, 1], 0.0))
            out_ref[v, b] = mine + theirs


ANY = pl.BlockSpec(memory_space=pl.ANY)


def merge(first, other, own, got, portion, bit, side):
    rows = own.shape[2] // 2
    cut = (1 << bit, rows >> bit)
    own, got = (t.reshape(4, 2, cut[0], 2, cut[1], PB) for t in (own, got))
    return pl.pallas_call(
        functools.partial(merge_body, portion=portion, side=side),
        in_specs=[SMEM, SMEM, ANY, ANY],
        out_specs=VMEM,
        out_shape=pltpu.VMEM((4, PBLK) + cut + (PB,), jnp.float32),
        scratch_shapes=[pltpu.VMEM((4, 2) + cut + (PB,), jnp.float32)] * 2 + [pltpu.SemaphoreType.DMA((8,))],
        cost_estimate=pl.CostEstimate(flops=1 << 30, transcendentals=0, bytes_accessed=2 << 20),
        compiler_params=vmem_params(4),
        name="merge_send" if side else "merge_keep",
    )(first, other, in_hbm(own), got)


def detect(table_ref, sums, passed):
    for e in range(EBINS):
        row = [table_ref[16 * e + m : 16 * e + m + 1, :] for m in range(MATS)]
        power = sums[0] * row[0]
        for m in range(1, MATS):
            power = power + sums[m] * row[m]
        passed[e] = jnp.exp(power)
    bins = [None] * CBINS
    for e in range(EBINS):
        value = passed[e]
        for c in range(CBINS):
            part = table_ref[16 * e + 4 + c : 16 * e + 5 + c, :] * value
            bins[c] = part if e == 0 else bins[c] + part
    return bins


DETECT_COST = pl.CostEstimate(flops=1 << 31, transcendentals=1 << 20, bytes_accessed=1 << 20)


def inner_body(cross_ref, place_ref, table_ref, sums_ref, near_ref, partial_ref, passed, passed_near):
    core = place_ref[0]

    def block(b, carry):
        own = detect(table_ref, [sums_ref[m, :, b] for m in range(MATS)], passed)
        near = detect(table_ref, [near_ref[m, b] for m in range(MATS)], passed_near)
        for c in range(CBINS):
            leak = cross_ref[c]
            for row in (0, 1):
                side = jnp.where(core == 1 - row, near[c], 0.0)
                partial_ref[c, row, b] = (1.0 - 2.0 * leak) * own[c][row] + leak * (own[c][1 - row] + side)
        return carry

    lax.fori_loop(0, PBLK, block, 0)


def inner(crosstalk, place, table, sums, near):
    rows = jax.ShapeDtypeStruct((CBINS,) + sums.shape[1:], jnp.float32)
    return pl.pallas_call(
        inner_body,
        in_specs=[SMEM] * 2 + [VMEM] * 3,
        out_specs=VMEM,
        out_shape=rows,
        scratch_shapes=[pltpu.VMEM((EBINS, 2, 16, PB), jnp.float32), pltpu.VMEM((EBINS, 16, PB), jnp.float32)],
        cost_estimate=DETECT_COST,
        compiler_params=vmem_params(8),
        name="inner",
    )(crosstalk, place, table, sums, near)


def finish_body(cross_ref, place_ref, table_ref, far_ref, partial_ref, out_ref, passed):
    core, present = place_ref[0], place_ref[1]

    def block(b, carry):
        far = detect(table_ref, [far_ref[m, b] for m in range(MATS)], passed)
        columns = pl.ds(pl.multiple_of(b * PB, PB), PB)
        for c in range(CBINS):
            side = cross_ref[c] * jnp.where(present == 1, far[c], 0.0)
            out_ref[c, core, :, columns] = partial_ref[c, core, b] + side
            out_ref[c, 1 - core, :, columns] = partial_ref[c, 1 - core, b]
        return carry

    lax.fori_loop(0, PBLK, block, 0)


def finish(crosstalk, place, table, far, partial):
    return pl.pallas_call(
        finish_body,
        in_specs=[SMEM] * 2 + [VMEM] * 3,
        out_specs=VMEM,
        out_shape=jax.ShapeDtypeStruct((CBINS, 2, 16, PBLK * PB), jnp.float32),
        scratch_shapes=[pltpu.VMEM((EBINS, 16, PB), jnp.float32)],
        cost_estimate=DETECT_COST,
        compiler_params=vmem_params(8),
        name="finish",
    )(crosstalk, place, table, far, partial)


def per_device(volume, system, geometry, attenuation, response, crosstalk):
    rows = volume.shape[1]
    depth = volume.shape[3]
    tile = lax.axis_index(TILE_AXES)
    vol = volume.reshape(rows, depth)
    order = row_order(rows)[:, None]
    matrix = system.reshape(depth, 32, PB)
    mine = lax.dynamic_index_in_dim(geometry, tile, 0, keepdims=False)
    partner = lax.dynamic_index_in_dim(geometry, tile ^ 1, 0, keepdims=False)

    own, away, columns, *rest = project_first(order, vol, matrix)
    crossing = [None] * 4
    current = [None] * 4

    def cross(w, own, away):
        crossing[w] = own, lax.ppermute(away, "core", [(0, 1), (1, 0)])

    def first_send(w):
        axis, which = ORDERS[w][0]
        return merge(mine, partner, *crossing[w], w, DIM_OF[axis, which] - 2, 1).astype(jnp.float16)

    cross(0, own, away)
    cross(1, *project(columns, rest[0]))
    cross(2, *project(columns, rest[1]))
    sends = [first_send(0)]
    sends[0], columns = lax.optimization_barrier((sends[0], columns))
    last = project(columns, rest[2])
    cross(3, *last)
    sends += [first_send(w) for w in range(1, 4)]
    keeps, sends[3] = lax.optimization_barrier((crossing, sends[3]))
    for w in range(4):
        axis, which = ORDERS[w][0]
        bit = DIM_OF[axis, which] - 2
        shape = [4, PBLK, 2, 2, 2, 2, 16, PB]
        shape[2 + bit] = 1
        got = lax.ppermute(sends[w], axis, PAIRS[which])
        keep = merge(mine, partner, *keeps[w], w, bit, 0)
        current[w] = [keep.reshape(shape), got.reshape(shape)]

    def total(parts):
        value = parts[0]
        for part in parts[1:]:
            value = value + part.astype(jnp.float32)
        return value

    for n in range(1, 4):
        sends = []
        for w in range(4):
            axis, which = ORDERS[w][n]
            dim = DIM_OF[axis, which]
            sent = total([lax.slice_in_dim(t, 1, 2, axis=dim) for t in current[w]]).astype(jnp.float16)
            current[w] = [lax.slice_in_dim(t, 0, 1, axis=dim) for t in current[w]]
            if n == 1:
                sent, kept = lax.optimization_barrier((sent, total(current[w])))
                current[w] = [kept]
            sends.append(sent)
        for w in range(4):
            axis, which = ORDERS[w][n]
            current[w].append(lax.ppermute(sends[w], axis, PAIRS[which]))
    for w in range(4):
        current[w] = total(current[w]).astype(jnp.float16)

    whole = jnp.concatenate([c.reshape(4, PBLK, MATS, 2, 2, PB) for c in current], axis=0)
    outgoing = whole.transpose(3, 2, 4, 1, 0, 5).reshape(8, 2, 64, PB)
    received = lax.all_to_all(outgoing, ("zh", "mat"), 0, 0, tiled=True)
    received = received.reshape(2, MATS, 2, PBLK, 16, PB).astype(jnp.float32)
    sums = received[0] + received[1]

    core = lax.axis_index("core")
    rounded = sums.astype(jnp.float16)
    top, bottom = rounded[:, 0], rounded[:, 1]
    axes = ("mat",) + TILE_AXES
    count = lax.axis_size(axes)
    me = lax.axis_index(axes)
    swap = [(i, i + 1) for i in range(1, count - 1, 2)]
    near = lax.ppermute(jnp.where(core == 0, bottom, top), "core", [(0, 1), (1, 0)])
    far = lax.ppermute(jnp.where(core == 0, top, bottom), axes, swap + [(j, i) for i, j in swap])
    present = jnp.logical_and(me > 0, me < count - 1).astype(jnp.int32)
    place = jnp.stack([core, present])
    table = jnp.concatenate([-attenuation.T, response.T, jnp.zeros((EBINS, 4), jnp.float32)], axis=1)
    table = jnp.broadcast_to(table.reshape(16 * EBINS, 1), (16 * EBINS, PB))
    partial = inner(crosstalk, place, table, sums, near.astype(jnp.float32))
    return finish(crosstalk, place, table, far.astype(jnp.float32), partial)


def solution(mesh):
    fine = Mesh(mesh.devices.reshape(4, 4, 2, 4, 2), AXES)
    in_specs = (P("mat", None, TILE_AXES, None), P(TILE_AXES, None, None, None), P(), P(), P(), P())
    out_specs = P(None, AXES, None, None)

    return jax.shard_map(per_device, mesh=fine, in_specs=in_specs, out_specs=out_specs, check_vma=False)
```

```python
import functools

import jax
import jax.numpy as jnp
from jax import lax
from jax.experimental import pallas as pl
from jax.experimental.pallas import tpu as pltpu
from jax.sharding import Mesh, PartitionSpec as P

PB = 128
PBLK = 4
CBINS = 8
EBINS = 64
MATS = 4
AXES = ("mat", "y", "zh", "x", "core")
TILE_AXES = ("y", "zh", "x", "core")
PAIRS = ([(0, 1), (1, 0), (2, 3), (3, 2)], [(1, 2), (2, 1), (3, 0), (0, 3)])
ORDERS = (
    (("x", 0), ("y", 0), ("x", 1), ("y", 1)),
    (("x", 1), ("y", 1), ("x", 0), ("y", 0)),
    (("y", 0), ("x", 0), ("y", 1), ("x", 1)),
    (("y", 1), ("x", 1), ("y", 0), ("x", 0)),
)
DIM_OF = {("x", 0): 2, ("x", 1): 3, ("y", 0): 4, ("y", 1): 5}


def pair_bits(i):
    return ((i + 1) // 2) % 2, i // 2


def row_order(slice_count):
    pos = jnp.arange(slice_count, dtype=jnp.int32)
    bits = [(pos // (256 >> n)) % 2 for n in range(5)]
    rest = pos % 16
    core = bits[0] ^ lax.axis_index("core")

    def place(b0, b1, name):
        mine = pair_bits(lax.axis_index(name))
        b0, b1 = b0 ^ mine[0], b1 ^ mine[1]
        return 2 * b1 + (b0 ^ b1)

    x = place(bits[1], bits[2], "x")
    y = place(bits[3], bits[4], "y")
    mat, zh, r = rest // 4, (rest // 2) % 2, rest % 2
    return mat * 128 + y * 32 + zh * 16 + x * 4 + core * 2 + r


def vmem_params(mib):
    return pltpu.CompilerParams(vmem_limit_bytes=mib << 20)


VMEM = pl.BlockSpec(memory_space=pltpu.VMEM)
SMEM = pl.BlockSpec(memory_space=pltpu.SMEM)
HBM = pl.BlockSpec(memory_space=pltpu.HBM)


def multiply(columns, matrix_ref, own_hbm, away_hbm, buf, sems):
    weights = jnp.swapaxes(matrix_ref[...], 0, 1)
    half = columns.shape[0] // 2
    copies = []
    for v in range(4):
        pair = jnp.concatenate([weights[2 * v], weights[2 * v + 1]], axis=1)
        got = jnp.dot(columns, pair, preferred_element_type=jnp.float32)
        buf[v, 0] = got[:, :PB]
        buf[v, 1] = got[:, PB:]
        copies.append(pltpu.make_async_copy(buf.at[v, :, pl.ds(half, half), :], away_hbm.at[v], sems.at[2 * v]))
        copies.append(pltpu.make_async_copy(buf.at[v, :, pl.ds(0, half), :], own_hbm.at[v], sems.at[2 * v + 1]))
        copies[-2].start()
        copies[-1].start()
    return copies


def wait_all(copies):
    for copy in copies:
        copy.wait()


def first_body(
    order_ref, vol_hbm, sys_hbm, own_hbm, away_hbm, col_ref, m1_ref, m2_ref, m3_ref, vol_buf, m0_buf, buf, sems, out_sems
):
    copies = [pltpu.make_async_copy(vol_hbm, vol_buf, sems.at[4])]
    for w, target in enumerate((m0_buf, m1_ref, m2_ref, m3_ref)):
        copies.append(pltpu.make_async_copy(sys_hbm.at[:, pl.ds(8 * w, 8), :], target, sems.at[w]))
    for copy in copies:
        copy.start()
    rows = vol_buf.shape[0]
    chosen = (order_ref[...] == lax.broadcasted_iota(jnp.int32, (rows, rows), 1)).astype(jnp.bfloat16)
    copies[0].wait()
    columns = jnp.dot(chosen, vol_buf[...], preferred_element_type=jnp.float32).astype(jnp.bfloat16)
    col_ref[...] = columns
    copies[1].wait()
    outs = multiply(columns, m0_buf, own_hbm, away_hbm, buf, out_sems)
    wait_all(copies[2:])
    wait_all(outs)


def in_hbm(x):
    return pltpu.with_memory_space_constraint(x, pltpu.HBM)


def in_vmem(x):
    return pltpu.with_memory_space_constraint(x, pltpu.VMEM)


def project_first(order, vol, matrix):
    rows, depth = vol.shape
    half = pltpu.HBM((4, 2, rows // 2, PB), jnp.float32)
    part = pltpu.VMEM((depth, 8, PB), jnp.bfloat16)
    return pl.pallas_call(
        first_body,
        in_specs=[VMEM, HBM, HBM],
        out_specs=[HBM] * 2 + [VMEM] * 4,
        out_shape=[half, half, pltpu.VMEM((rows, depth), jnp.bfloat16), part, part, part],
        scratch_shapes=[
            pltpu.VMEM((rows, depth), jnp.bfloat16),
            pltpu.VMEM((depth, 8, PB), jnp.bfloat16),
            pltpu.VMEM((4, 2, rows, PB), jnp.float32),
            pltpu.SemaphoreType.DMA((5,)),
            pltpu.SemaphoreType.DMA((8,)),
        ],
        cost_estimate=pl.CostEstimate(flops=2 * rows * depth * 12 * PB, transcendentals=0, bytes_accessed=12 << 20),
        compiler_params=vmem_params(16),
        name="project_first",
    )(order, in_hbm(vol), in_hbm(matrix))


def project_body(col_ref, *refs):
    matrices, outs, bufs, sems = refs[:3], refs[3:9], refs[9:12], refs[12:]
    columns = col_ref[...]
    copies = []
    for i in range(3):
        copies += multiply(columns, matrices[i], outs[2 * i], outs[2 * i + 1], bufs[i], sems[i])
    wait_all(copies)


def project(columns, matrices):
    rows, depth = columns.shape
    half = pltpu.HBM((4, 2, rows // 2, PB), jnp.float32)
    got = pl.pallas_call(
        project_body,
        in_specs=[VMEM] * 4,
        out_specs=[HBM] * 6,
        out_shape=[half] * 6,
        scratch_shapes=[pltpu.VMEM((4, 2, rows, PB), jnp.float32)] * 3 + [pltpu.SemaphoreType.DMA((8,))] * 3,
        cost_estimate=pl.CostEstimate(flops=6 * rows * depth * 8 * PB, transcendentals=0, bytes_accessed=15 << 20),
        compiler_params=vmem_params(14),
        name="project",
    )(in_vmem(columns), *[in_vmem(m) for m in matrices])
    return got[0:2], got[2:4], got[4:6]


def merge_body(first_ref, other_ref, own_any, got_any, out_ref, own_buf, got_buf, sems, *, portion, side):
    copies = []
    for v in range(4):
        copies.append(pltpu.make_async_copy(own_any.at[v, :, :, side], own_buf.at[v], sems.at[2 * v]))
        copies.append(pltpu.make_async_copy(got_any.at[v, :, :, side], got_buf.at[v], sems.at[2 * v + 1]))
    for copy in copies:
        copy.start()
    for v in range(4):
        wait_all(copies[2 * v : 2 * v + 2])
        first, other = first_ref[4 * portion + v], other_ref[4 * portion + v]
        for b in range(PBLK):
            mine = jnp.where(first == b, own_buf[v, 0], jnp.where(first + 1 == b, own_buf[v, 1], 0.0))
            theirs = jnp.where(other == b, got_buf[v, 0], jnp.where(other + 1 == b, got_buf[v, 1], 0.0))
            out_ref[v, b] = mine + theirs


ANY = pl.BlockSpec(memory_space=pl.ANY)


def merge(first, other, own, got, portion, bit, side):
    rows = own.shape[2] // 2
    cut = (1 << bit, rows >> bit)
    own, got = (t.reshape(4, 2, cut[0], 2, cut[1], PB) for t in (own, got))
    return pl.pallas_call(
        functools.partial(merge_body, portion=portion, side=side),
        in_specs=[SMEM, SMEM, ANY, ANY],
        out_specs=VMEM,
        out_shape=pltpu.VMEM((4, PBLK) + cut + (PB,), jnp.float32),
        scratch_shapes=[pltpu.VMEM((4, 2) + cut + (PB,), jnp.float32)] * 2 + [pltpu.SemaphoreType.DMA((8,))],
        cost_estimate=pl.CostEstimate(flops=1 << 30, transcendentals=0, bytes_accessed=2 << 20),
        compiler_params=vmem_params(4),
        name="merge_send" if side else "merge_keep",
    )(first, other, own, got)


def detect(natt_ref, resp_ref, sums):
    high, low = [], []
    for v in range(16):
        power = natt_ref[0] * sums[0][v : v + 1]
        for m in range(1, MATS):
            power = power + natt_ref[m] * sums[m][v : v + 1]
        passed = jnp.exp(power)
        top = passed.astype(jnp.bfloat16)
        high.append(top)
        low.append((passed - top.astype(jnp.float32)).astype(jnp.bfloat16))
    terms = jnp.concatenate([jnp.concatenate(high, axis=1), jnp.concatenate(low, axis=1)], axis=0)
    got = jnp.dot(resp_ref[...], terms, preferred_element_type=jnp.float32)
    got = got[:CBINS] + got[CBINS:]
    return jnp.swapaxes(jnp.stack([got[:, v * PB : (v + 1) * PB] for v in range(16)]), 0, 1)


def split_response(response):
    top = lax.reduce_precision(response, 8, 7)
    rest = response - top
    rows = jnp.concatenate([jnp.concatenate([top, top], axis=1), jnp.pad(rest, ((0, 0), (0, EBINS)))], axis=0)
    return rows.astype(jnp.bfloat16)


DETECT_COST = pl.CostEstimate(flops=1 << 31, transcendentals=1 << 20, bytes_accessed=1 << 20)


def inner_body(cross_ref, place_ref, natt_ref, resp_ref, sums_ref, near_ref, partial_ref):
    core = place_ref[0]

    def block(b, carry):
        own = [detect(natt_ref, resp_ref, [sums_ref[m, r, b] for m in range(MATS)]) for r in (0, 1)]
        near = detect(natt_ref, resp_ref, [near_ref[m, b] for m in range(MATS)])
        for c in range(CBINS):
            leak = cross_ref[c]
            for row in (0, 1):
                side = jnp.where(core == 1 - row, near[c], 0.0)
                partial_ref[c, row, b] = (1.0 - 2.0 * leak) * own[row][c] + leak * (own[1 - row][c] + side)
        return carry

    lax.fori_loop(0, PBLK, block, 0)


def inner(crosstalk, place, natt, resp, sums, near):
    return pl.pallas_call(
        inner_body,
        in_specs=[SMEM] * 2 + [VMEM] * 4,
        out_specs=VMEM,
        out_shape=jax.ShapeDtypeStruct((CBINS,) + sums.shape[1:], jnp.float32),
        cost_estimate=DETECT_COST,
        compiler_params=vmem_params(8),
        name="inner",
    )(crosstalk, place, natt, resp, sums, near)


def finish_body(cross_ref, place_ref, natt_ref, resp_ref, far_ref, partial_ref, out_ref):
    core, present = place_ref[0], place_ref[1]

    def block(b, carry):
        far = detect(natt_ref, resp_ref, [far_ref[m, b] for m in range(MATS)])
        columns = pl.ds(pl.multiple_of(b * PB, PB), PB)
        for c in range(CBINS):
            side = cross_ref[c] * jnp.where(present == 1, far[c], 0.0)
            out_ref[c, core, :, columns] = partial_ref[c, core, b] + side
            out_ref[c, 1 - core, :, columns] = partial_ref[c, 1 - core, b]
        return carry

    lax.fori_loop(0, PBLK, block, 0)


def finish(crosstalk, place, natt, resp, far, partial):
    return pl.pallas_call(
        finish_body,
        in_specs=[SMEM] * 2 + [VMEM] * 4,
        out_specs=VMEM,
        out_shape=jax.ShapeDtypeStruct((CBINS, 2, 16, PBLK * PB), jnp.float32),
        cost_estimate=DETECT_COST,
        compiler_params=vmem_params(8),
        name="finish",
    )(crosstalk, place, natt, resp, far, partial)


def per_device(volume, system, geometry, attenuation, response, crosstalk):
    rows = volume.shape[1]
    depth = volume.shape[3]
    tile = lax.axis_index(TILE_AXES)
    vol = volume.reshape(rows, depth)
    order = row_order(rows)[:, None]
    matrix = system.reshape(depth, 32, PB)
    mine = lax.dynamic_index_in_dim(geometry, tile, 0, keepdims=False)
    partner = lax.dynamic_index_in_dim(geometry, tile ^ 1, 0, keepdims=False)

    own, away, columns, *rest = project_first(order, vol, matrix)
    crossing = [None] * 4
    current = [None] * 4

    def cross(w, own, away):
        crossing[w] = own, lax.ppermute(away, "core", [(0, 1), (1, 0)])

    def first_send(w):
        axis, which = ORDERS[w][0]
        return merge(mine, partner, *crossing[w], w, DIM_OF[axis, which] - 2, 1).astype(jnp.float16)

    cross(0, own, away)
    others = project(columns, rest)
    for w in range(1, 4):
        cross(w, *others[w - 1])
    sends = [first_send(w) for w in range(4)]
    keeps, sends[3] = lax.optimization_barrier((crossing, sends[3]))
    for w in range(4):
        axis, which = ORDERS[w][0]
        bit = DIM_OF[axis, which] - 2
        shape = [4, PBLK, 2, 2, 2, 2, 16, PB]
        shape[2 + bit] = 1
        got = lax.ppermute(sends[w], axis, PAIRS[which])
        keep = merge(mine, partner, *keeps[w], w, bit, 0)
        current[w] = [keep.reshape(shape), got.reshape(shape)]

    def total(parts):
        value = parts[0]
        for part in parts[1:]:
            value = value + part.astype(jnp.float32)
        return value

    for n in range(1, 4):
        sends = []
        for w in range(4):
            axis, which = ORDERS[w][n]
            dim = DIM_OF[axis, which]
            sent = total([lax.slice_in_dim(t, 1, 2, axis=dim) for t in current[w]]).astype(jnp.float16)
            current[w] = [lax.slice_in_dim(t, 0, 1, axis=dim) for t in current[w]]
            if n == 1:
                sent, kept = lax.optimization_barrier((sent, total(current[w])))
                current[w] = [kept]
            sends.append(sent)
        for w in range(4):
            axis, which = ORDERS[w][n]
            current[w].append(lax.ppermute(sends[w], axis, PAIRS[which]))
    for w in range(4):
        current[w] = total(current[w]).astype(jnp.float16)

    whole = jnp.concatenate([c.reshape(4, PBLK, MATS, 2, 2, PB) for c in current], axis=0)
    outgoing = whole.transpose(3, 2, 4, 1, 0, 5).reshape(8, 2, 64, PB)
    received = lax.all_to_all(outgoing, ("zh", "mat"), 0, 0, tiled=True)
    received = received.reshape(2, MATS, 2, PBLK, 16, PB).astype(jnp.float32)
    sums = received[0] + received[1]

    core = lax.axis_index("core")
    rounded = sums.astype(jnp.float16)
    top, bottom = rounded[:, 0], rounded[:, 1]
    axes = ("mat",) + TILE_AXES
    count = lax.axis_size(axes)
    me = lax.axis_index(axes)
    swap = [(i, i + 1) for i in range(1, count - 1, 2)]
    near = lax.ppermute(jnp.where(core == 0, bottom, top), "core", [(0, 1), (1, 0)])
    far = lax.ppermute(jnp.where(core == 0, top, bottom), axes, swap + [(j, i) for i, j in swap])
    present = jnp.logical_and(me > 0, me < count - 1).astype(jnp.int32)
    place = jnp.stack([core, present])
    natt = jnp.broadcast_to(-attenuation[:, :, None], (MATS, EBINS, PB))
    resp = split_response(response)
    partial = inner(crosstalk, place, natt, resp, sums, near.astype(jnp.float32))
    return finish(crosstalk, place, natt, resp, far.astype(jnp.float32), partial)


def solution(mesh):
    fine = Mesh(mesh.devices.reshape(4, 4, 2, 4, 2), AXES)
    in_specs = (P("mat", None, TILE_AXES, None), P(TILE_AXES, None, None, None), P(), P(), P(), P())
    out_specs = P(None, AXES, None, None)

    return jax.shard_map(per_device, mesh=fine, in_specs=in_specs, out_specs=out_specs, check_vma=False)
```

```python
import functools

import jax
import jax.numpy as jnp
from jax import lax
from jax.experimental import pallas as pl
from jax.experimental.pallas import tpu as pltpu
from jax.sharding import Mesh, PartitionSpec as P

PB = 128
PBLK = 4
CBINS = 8
EBINS = 64
MATS = 4
AXES = ("mat", "y", "zh", "x", "core")
TILE_AXES = ("y", "zh", "x", "core")
PAIRS = ([(0, 1), (1, 0), (2, 3), (3, 2)], [(1, 2), (2, 1), (3, 0), (0, 3)])
ORDERS = (
    (("x", 0), ("x", 1), ("y", 0), ("y", 1)),
    (("x", 1), ("x", 0), ("y", 1), ("y", 0)),
    (("y", 0), ("y", 1), ("x", 0), ("x", 1)),
    (("y", 1), ("y", 0), ("x", 1), ("x", 0)),
)
FIRST_BIT = (0, 1, 2, 3)
DIM_OF = {("x", 0): 2, ("x", 1): 3, ("y", 0): 4, ("y", 1): 5}


SEND_GROUPS = ((0,), (1,), (2,), (3,))
KEEP_GROUPS = ((0, 1, 2, 3),)


def pair_bits(i):
    return ((i + 1) // 2) % 2, i // 2


def row_order(slice_count):
    pos = jnp.arange(slice_count, dtype=jnp.int32)
    bits = [(pos // (256 >> n)) % 2 for n in range(5)]
    rest = pos % 16
    core = bits[0] ^ lax.axis_index("core")

    def place(b0, b1, name):
        mine = pair_bits(lax.axis_index(name))
        b0, b1 = b0 ^ mine[0], b1 ^ mine[1]
        return 2 * b1 + (b0 ^ b1)

    x = place(bits[1], bits[2], "x")
    y = place(bits[3], bits[4], "y")
    mat, zh, r = rest // 4, (rest // 2) % 2, rest % 2
    return mat * 128 + y * 32 + zh * 16 + x * 4 + core * 2 + r


def vmem_params(mib):
    return pltpu.CompilerParams(vmem_limit_bytes=mib << 20)


VMEM = pl.BlockSpec(memory_space=pltpu.VMEM)
SMEM = pl.BlockSpec(memory_space=pltpu.SMEM)
HBM = pl.BlockSpec(memory_space=pltpu.HBM)


def multiply(columns, matrix_ref, own_hbm, away_hbm, buf, sems):
    weights = jnp.swapaxes(matrix_ref[...], 0, 1)
    half = columns.shape[0] // 2
    copies = []
    for v in range(4):
        pair = jnp.concatenate([weights[2 * v], weights[2 * v + 1]], axis=1)
        got = jnp.dot(columns, pair, preferred_element_type=jnp.float32)
        buf[v, 0] = got[:, :PB]
        buf[v, 1] = got[:, PB:]
        copies.append(pltpu.make_async_copy(buf.at[v, :, pl.ds(half, half), :], away_hbm.at[v], sems.at[2 * v]))
        copies.append(pltpu.make_async_copy(buf.at[v, :, pl.ds(0, half), :], own_hbm.at[v], sems.at[2 * v + 1]))
        copies[-2].start()
        copies[-1].start()
    return copies


def wait_all(copies):
    for copy in copies:
        copy.wait()


def first_body(
    order_ref, vol_hbm, sys_hbm, own_hbm, away_hbm, col_ref, m1_ref, m2_ref, m3_ref, vol_buf, m0_buf, buf, sems, out_sems
):
    copies = [pltpu.make_async_copy(vol_hbm, vol_buf, sems.at[4])]
    for w, target in enumerate((m0_buf, m1_ref, m2_ref, m3_ref)):
        copies.append(pltpu.make_async_copy(sys_hbm.at[:, pl.ds(8 * w, 8), :], target, sems.at[w]))
    for copy in copies:
        copy.start()
    rows = vol_buf.shape[0]
    chosen = (order_ref[...] == lax.broadcasted_iota(jnp.int32, (rows, rows), 1)).astype(jnp.bfloat16)
    copies[0].wait()
    columns = jnp.dot(chosen, vol_buf[...], preferred_element_type=jnp.float32).astype(jnp.bfloat16)
    col_ref[...] = columns
    copies[1].wait()
    outs = multiply(columns, m0_buf, own_hbm, away_hbm, buf, out_sems)
    wait_all(copies[2:])
    wait_all(outs)


def in_hbm(x):
    return pltpu.with_memory_space_constraint(x, pltpu.HBM)


def in_vmem(x):
    return pltpu.with_memory_space_constraint(x, pltpu.VMEM)


def project_first(order, vol, matrix):
    rows, depth = vol.shape
    half = pltpu.HBM((4, 2, rows // 2, PB), jnp.float32)
    part = pltpu.VMEM((depth, 8, PB), jnp.bfloat16)
    return pl.pallas_call(
        first_body,
        in_specs=[VMEM, HBM, HBM],
        out_specs=[HBM] * 2 + [VMEM] * 4,
        out_shape=[half, half, pltpu.VMEM((rows, depth), jnp.bfloat16), part, part, part],
        scratch_shapes=[
            pltpu.VMEM((rows, depth), jnp.bfloat16),
            pltpu.VMEM((depth, 8, PB), jnp.bfloat16),
            pltpu.VMEM((4, 2, rows, PB), jnp.float32),
            pltpu.SemaphoreType.DMA((5,)),
            pltpu.SemaphoreType.DMA((8,)),
        ],
        cost_estimate=pl.CostEstimate(flops=2 * rows * depth * 12 * PB, transcendentals=0, bytes_accessed=12 << 20),
        compiler_params=vmem_params(16),
        name="project_first",
    )(order, in_hbm(vol), in_hbm(matrix))


def project_body(col_ref, *refs):
    matrices, outs, bufs, sems = refs[:3], refs[3:9], refs[9:12], refs[12:]
    columns = col_ref[...]
    copies = []
    for i in range(3):
        copies += multiply(columns, matrices[i], outs[2 * i], outs[2 * i + 1], bufs[i], sems[i])
    wait_all(copies)


def project(columns, matrices):
    rows, depth = columns.shape
    half = pltpu.HBM((4, 2, rows // 2, PB), jnp.float32)
    got = pl.pallas_call(
        project_body,
        in_specs=[VMEM] * 4,
        out_specs=[HBM] * 6,
        out_shape=[half] * 6,
        scratch_shapes=[pltpu.VMEM((4, 2, rows, PB), jnp.float32)] * 3 + [pltpu.SemaphoreType.DMA((8,))] * 3,
        cost_estimate=pl.CostEstimate(flops=6 * rows * depth * 8 * PB, transcendentals=0, bytes_accessed=15 << 20),
        compiler_params=vmem_params(14),
        name="project",
    )(in_vmem(columns), *[in_vmem(m) for m in matrices])
    return got[0:2], got[2:4], got[4:6]


def merge_body(first_ref, other_ref, *refs, portions, side):
    count = len(portions)
    own, got, out = refs[:count], refs[count : 2 * count], refs[2 * count : 3 * count]
    own_buf, got_buf, sems = refs[3 * count : 4 * count], refs[4 * count : 5 * count], refs[5 * count]
    copies = []
    for i in range(count):
        for v in range(4):
            place = 8 * i + 2 * v
            copies.append(pltpu.make_async_copy(own[i].at[v, :, :, side], own_buf[i].at[v], sems.at[place]))
            copies.append(pltpu.make_async_copy(got[i].at[v, :, :, side], got_buf[i].at[v], sems.at[place + 1]))
    for copy in copies:
        copy.start()
    for i, portion in enumerate(portions):
        for v in range(4):
            wait_all(copies[8 * i + 2 * v : 8 * i + 2 * v + 2])
            view = 4 * portion + v
            first, other = first_ref[view : view + 1], other_ref[view : view + 1]
            for b in range(PBLK):
                low, high = own_buf[i][v, 0], own_buf[i][v, 1]
                mine = jnp.where(first == b, low, jnp.where(first + 1 == b, high, 0.0))
                low, high = got_buf[i][v, 0], got_buf[i][v, 1]
                out[i][v, b] = mine + jnp.where(other == b, low, jnp.where(other + 1 == b, high, 0.0))


ANY = pl.BlockSpec(memory_space=pl.ANY)


def merge(first, other, crossing, portions, side):
    rows = crossing[0][0].shape[2] // 2
    cuts = [(1 << FIRST_BIT[w], rows >> FIRST_BIT[w]) for w in portions]
    count = len(portions)
    inputs = [crossing[w][k].reshape(4, 2, c[0], 2, c[1], PB) for k in range(2) for w, c in zip(portions, cuts)]
    buffers = [pltpu.VMEM((4, 2) + c + (PB,), jnp.float32) for c in cuts]
    return pl.pallas_call(
        functools.partial(merge_body, portions=portions, side=side),
        in_specs=[VMEM, VMEM] + [ANY] * (2 * count),
        out_specs=[VMEM] * count,
        out_shape=[pltpu.VMEM((4, PBLK) + c + (PB,), jnp.float32) for c in cuts],
        scratch_shapes=buffers * 2 + [pltpu.SemaphoreType.DMA((8 * count,))],
        cost_estimate=pl.CostEstimate(flops=count << 30, transcendentals=0, bytes_accessed=count << 21),
        compiler_params=vmem_params(3 * count + 1),
        name="merge_send" if side else "merge_keep",
    )(first, other, *inputs)


def detect(natt_ref, resp_ref, sums):
    high, low = [], []
    for v in range(16):
        power = natt_ref[0] * sums[0][v : v + 1]
        for m in range(1, MATS):
            power = power + natt_ref[m] * sums[m][v : v + 1]
        passed = jnp.exp(power)
        top = passed.astype(jnp.bfloat16)
        high.append(top)
        low.append((passed - top.astype(jnp.float32)).astype(jnp.bfloat16))
    terms = jnp.concatenate([jnp.concatenate(high, axis=1), jnp.concatenate(low, axis=1)], axis=0)
    got = jnp.dot(resp_ref[...], terms, preferred_element_type=jnp.float32)
    got = got[:CBINS] + got[CBINS:]
    return jnp.swapaxes(jnp.stack([got[:, v * PB : (v + 1) * PB] for v in range(16)]), 0, 1)


def split_response(response):
    top = lax.reduce_precision(response, 8, 7)
    rest = response - top
    rows = jnp.concatenate([jnp.concatenate([top, top], axis=1), jnp.pad(rest, ((0, 0), (0, EBINS)))], axis=0)
    return rows.astype(jnp.bfloat16)


DETECT_COST = pl.CostEstimate(flops=1 << 31, transcendentals=1 << 20, bytes_accessed=1 << 20)


def inner_body(cross_ref, near_share_ref, natt_ref, resp_ref, sums_ref, near_ref, partial_ref):
    def block(b, carry):
        own = [detect(natt_ref, resp_ref, [sums_ref[m, r, b] for m in range(MATS)]) for r in (0, 1)]
        near = detect(natt_ref, resp_ref, [near_ref[m, b] for m in range(MATS)])
        for c in range(CBINS):
            leak = cross_ref[c : c + 1]
            for row in (0, 1):
                share = near_share_ref[row, c : c + 1]
                side = jnp.where(share > 0.0, share * near[c], 0.0)
                partial_ref[c, row, b] = (1.0 - 2.0 * leak) * own[row][c] + leak * own[1 - row][c] + side
        return carry

    lax.fori_loop(0, PBLK, block, 0)


def inner(leak, share, natt, resp, sums, near):
    return pl.pallas_call(
        inner_body,
        in_specs=[VMEM] * 6,
        out_specs=VMEM,
        out_shape=jax.ShapeDtypeStruct((CBINS,) + sums.shape[1:], jnp.float32),
        cost_estimate=DETECT_COST,
        compiler_params=vmem_params(8),
        name="inner",
    )(leak, share, natt, resp, sums, near)


def finish_body(far_share_ref, natt_ref, resp_ref, far_ref, partial_ref, out_ref):
    def block(b, carry):
        far = detect(natt_ref, resp_ref, [far_ref[m, b] for m in range(MATS)])
        columns = pl.ds(pl.multiple_of(b * PB, PB), PB)
        for c in range(CBINS):
            for row in (0, 1):
                share = far_share_ref[row, c : c + 1]
                out_ref[c, row, :, columns] = partial_ref[c, row, b] + jnp.where(share > 0.0, share * far[c], 0.0)
        return carry

    lax.fori_loop(0, PBLK, block, 0)


def finish(share, natt, resp, far, partial):
    return pl.pallas_call(
        finish_body,
        in_specs=[VMEM] * 5,
        out_specs=VMEM,
        out_shape=jax.ShapeDtypeStruct((CBINS, 2, 16, PBLK * PB), jnp.float32),
        cost_estimate=DETECT_COST,
        compiler_params=vmem_params(8),
        name="finish",
    )(share, natt, resp, far, partial)


def per_device(volume, system, geometry, attenuation, response, crosstalk):
    rows = volume.shape[1]
    depth = volume.shape[3]
    tile = lax.axis_index(TILE_AXES)
    vol = volume.reshape(rows, depth)
    order = row_order(rows)[:, None]
    matrix = system.reshape(depth, 32, PB)
    mine = lax.dynamic_index_in_dim(geometry, tile, 0, keepdims=False)
    partner = lax.dynamic_index_in_dim(geometry, tile ^ 1, 0, keepdims=False)
    mine, partner = (jnp.broadcast_to(t[:, None], (16, PB)) for t in (mine, partner))

    own, away, columns, *rest = project_first(order, vol, matrix)
    crossing = [None] * 4
    current = [None] * 4

    def cross(w, own, away):
        crossing[w] = own, lax.ppermute(away, "core", [(0, 1), (1, 0)])

    cross(0, own, away)
    others = project(columns, rest)
    for w in range(1, 4):
        cross(w, *others[w - 1])
    sends = []
    for group in SEND_GROUPS:
        sends += [part.astype(jnp.float16) for part in merge(mine, partner, crossing, group, 1)]
    crossing, sends[3] = lax.optimization_barrier((crossing, sends[3]))
    keeps = []
    for group in KEEP_GROUPS:
        keeps += merge(mine, partner, crossing, group, 0)
    for w in range(4):
        axis, which = ORDERS[w][0]
        shape = [4, PBLK, 2, 2, 2, 2, 16, PB]
        shape[2 + FIRST_BIT[w]] = 1
        got = lax.ppermute(sends[w], axis, PAIRS[which])
        current[w] = [keeps[w].reshape(shape), got.reshape(shape)]

    def total(parts):
        value = parts[0]
        for part in parts[1:]:
            value = value + part.astype(jnp.float32)
        return value

    for n in range(1, 4):
        sends = []
        for w in range(4):
            axis, which = ORDERS[w][n]
            dim = DIM_OF[axis, which]
            sent = total([lax.slice_in_dim(t, 1, 2, axis=dim) for t in current[w]]).astype(jnp.float16)
            current[w] = [lax.slice_in_dim(t, 0, 1, axis=dim) for t in current[w]]
            if n == 1:
                sent, kept = lax.optimization_barrier((sent, total(current[w])))
                current[w] = [kept]
            sends.append(sent)
        for w in range(4):
            axis, which = ORDERS[w][n]
            current[w].append(lax.ppermute(sends[w], axis, PAIRS[which]))
    for w in range(4):
        current[w] = total(current[w]).astype(jnp.float16)

    whole = jnp.concatenate([c.reshape(4, PBLK, MATS, 2, 2, PB) for c in current], axis=0)
    outgoing = whole.transpose(3, 2, 4, 1, 0, 5).reshape(8, 2, 64, PB)
    received = lax.all_to_all(outgoing, ("zh", "mat"), 0, 0, tiled=True)
    received = received.reshape(2, MATS, 2, PBLK, 16, PB).astype(jnp.float32)
    sums = received[0] + received[1]

    core = lax.axis_index("core")
    rounded = sums.astype(jnp.float16)
    top, bottom = rounded[:, 0], rounded[:, 1]
    axes = ("mat",) + TILE_AXES
    count = lax.axis_size(axes)
    me = lax.axis_index(axes)
    swap = [(i, i + 1) for i in range(1, count - 1, 2)]
    near = lax.ppermute(jnp.where(core == 0, bottom, top), "core", [(0, 1), (1, 0)])
    far = lax.ppermute(jnp.where(core == 0, top, bottom), axes, swap + [(j, i) for i, j in swap])
    leak = jnp.broadcast_to(crosstalk[:, None], (CBINS, PB))
    present = jnp.logical_and(me > 0, me < count - 1)
    row = jnp.arange(2, dtype=jnp.int32)[:, None, None]
    near_share = jnp.where(row == 1 - core, leak, 0.0)
    far_share = jnp.where(jnp.logical_and(row == core, present), leak, 0.0)
    natt = jnp.broadcast_to(-attenuation[:, :, None], (MATS, EBINS, PB))
    resp = split_response(response)
    partial = inner(leak, near_share, natt, resp, sums, near.astype(jnp.float32))
    return finish(far_share, natt, resp, far.astype(jnp.float32), partial)


def solution(mesh):
    fine = Mesh(mesh.devices.reshape(4, 4, 2, 4, 2), AXES)
    in_specs = (P("mat", None, TILE_AXES, None), P(TILE_AXES, None, None, None), P(), P(), P(), P())
    out_specs = P(None, AXES, None, None)

    return jax.shard_map(per_device, mesh=fine, in_specs=in_specs, out_specs=out_specs, check_vma=False)
```

```python
import functools

import jax
import jax.numpy as jnp
from jax import lax
from jax.experimental import pallas as pl
from jax.experimental.pallas import tpu as pltpu
from jax.sharding import Mesh, PartitionSpec as P

PB = 128
PBLK = 4
CBINS = 8
EBINS = 64
MATS = 4
AXES = ("mat", "y", "zh", "x", "core")
TILE_AXES = ("y", "zh", "x", "core")
PAIRS = ([(0, 1), (1, 0), (2, 3), (3, 2)], [(1, 2), (2, 1), (3, 0), (0, 3)])
ORDERS = (
    (("x", 0), ("x", 1), ("y", 0), ("y", 1)),
    (("x", 1), ("x", 0), ("y", 1), ("y", 0)),
    (("y", 0), ("y", 1), ("x", 0), ("x", 1)),
    (("y", 1), ("y", 0), ("x", 1), ("x", 0)),
)
FIRST_BIT = (0, 1, 2, 3)
DIM_OF = {("x", 0): 2, ("x", 1): 3, ("y", 0): 4, ("y", 1): 5}


SEND_GROUPS = ((0,), (1,), (2,), (3,))
KEEP_GROUPS = ((0, 1, 2, 3),)


def pair_bits(i):
    return ((i + 1) >> 1) & 1, i >> 1


def row_order(slice_count):
    pos = lax.broadcasted_iota(jnp.int32, (slice_count, 1), 0)
    bits = [(pos >> (8 - n)) & 1 for n in range(5)]
    rest = pos & 15
    core = bits[0] ^ lax.axis_index("core")

    def place(b0, b1, name):
        mine = pair_bits(lax.axis_index(name))
        b0, b1 = b0 ^ mine[0], b1 ^ mine[1]
        return 2 * b1 + (b0 ^ b1)

    x = place(bits[1], bits[2], "x")
    y = place(bits[3], bits[4], "y")
    mat, zh, r = rest >> 2, (rest >> 1) & 1, rest & 1
    return mat * 128 + y * 32 + zh * 16 + x * 4 + core * 2 + r


def vmem_params(mib):
    return pltpu.CompilerParams(vmem_limit_bytes=mib << 20)


VMEM = pl.BlockSpec(memory_space=pltpu.VMEM)
SMEM = pl.BlockSpec(memory_space=pltpu.SMEM)
HBM = pl.BlockSpec(memory_space=pltpu.HBM)


def multiply(columns, matrix_ref, own_hbm, away_hbm, buf, sems):
    weights = jnp.swapaxes(matrix_ref[...], 0, 1)
    half = columns.shape[0] // 2
    copies = []
    for v in range(4):
        pair = jnp.concatenate([weights[2 * v], weights[2 * v + 1]], axis=1)
        got = jnp.dot(columns, pair, preferred_element_type=jnp.float32)
        buf[v, 0] = got[:, :PB]
        buf[v, 1] = got[:, PB:]
        copies.append(pltpu.make_async_copy(buf.at[v, :, pl.ds(half, half), :], away_hbm.at[v], sems.at[2 * v]))
        copies.append(pltpu.make_async_copy(buf.at[v, :, pl.ds(0, half), :], own_hbm.at[v], sems.at[2 * v + 1]))
        copies[-2].start()
        copies[-1].start()
    return copies


def wait_all(copies):
    for copy in copies:
        copy.wait()


def first_body(
    vol_hbm, sys_hbm, own_hbm, away_hbm, col_ref, m1_ref, m2_ref, m3_ref, vol_buf, m0_buf, buf, sems, out_sems
):
    copies = [pltpu.make_async_copy(vol_hbm, vol_buf, sems.at[4])]
    for w, target in enumerate((m0_buf, m1_ref, m2_ref, m3_ref)):
        copies.append(pltpu.make_async_copy(sys_hbm.at[:, pl.ds(8 * w, 8), :], target, sems.at[w]))
    for copy in copies:
        copy.start()
    rows = vol_buf.shape[0]
    chosen = (row_order(rows) == lax.broadcasted_iota(jnp.int32, (rows, rows), 1)).astype(jnp.bfloat16)
    copies[0].wait()
    columns = jnp.dot(chosen, vol_buf[...], preferred_element_type=jnp.float32).astype(jnp.bfloat16)
    col_ref[...] = columns
    copies[1].wait()
    outs = multiply(columns, m0_buf, own_hbm, away_hbm, buf, out_sems)
    wait_all(copies[2:])
    wait_all(outs)


def in_hbm(x):
    return pltpu.with_memory_space_constraint(x, pltpu.HBM)


def in_vmem(x):
    return pltpu.with_memory_space_constraint(x, pltpu.VMEM)


def project_first(vol, matrix):
    rows, depth = vol.shape
    half = pltpu.HBM((4, 2, rows // 2, PB), jnp.float32)
    part = pltpu.VMEM((depth, 8, PB), jnp.bfloat16)
    return pl.pallas_call(
        first_body,
        in_specs=[HBM, HBM],
        out_specs=[HBM] * 2 + [VMEM] * 4,
        out_shape=[half, half, pltpu.VMEM((rows, depth), jnp.bfloat16), part, part, part],
        scratch_shapes=[
            pltpu.VMEM((rows, depth), jnp.bfloat16),
            pltpu.VMEM((depth, 8, PB), jnp.bfloat16),
            pltpu.VMEM((4, 2, rows, PB), jnp.float32),
            pltpu.SemaphoreType.DMA((5,)),
            pltpu.SemaphoreType.DMA((8,)),
        ],
        cost_estimate=pl.CostEstimate(flops=2 * rows * depth * 12 * PB, transcendentals=0, bytes_accessed=12 << 20),
        compiler_params=vmem_params(16),
        name="project_first",
    )(in_hbm(vol), in_hbm(matrix))


def project_body(col_ref, *refs):
    matrices, outs, bufs, sems = refs[:3], refs[3:9], refs[9:12], refs[12:]
    columns = col_ref[...]
    copies = []
    for i in range(3):
        copies += multiply(columns, matrices[i], outs[2 * i], outs[2 * i + 1], bufs[i], sems[i])
    wait_all(copies)


def project(columns, matrices):
    rows, depth = columns.shape
    half = pltpu.HBM((4, 2, rows // 2, PB), jnp.float32)
    got = pl.pallas_call(
        project_body,
        in_specs=[VMEM] * 4,
        out_specs=[HBM] * 6,
        out_shape=[half] * 6,
        scratch_shapes=[pltpu.VMEM((4, 2, rows, PB), jnp.float32)] * 3 + [pltpu.SemaphoreType.DMA((8,))] * 3,
        cost_estimate=pl.CostEstimate(flops=6 * rows * depth * 8 * PB, transcendentals=0, bytes_accessed=15 << 20),
        compiler_params=vmem_params(14),
        name="project",
    )(in_vmem(columns), *[in_vmem(m) for m in matrices])
    return got[0:2], got[2:4], got[4:6]


def merge_body(first_ref, other_ref, *refs, portions, side):
    count = len(portions)
    own, got, out = refs[:count], refs[count : 2 * count], refs[2 * count : 3 * count]
    own_buf, got_buf, sems = refs[3 * count : 4 * count], refs[4 * count : 5 * count], refs[5 * count]
    copies = []
    for i in range(count):
        for v in range(4):
            place = 8 * i + 2 * v
            copies.append(pltpu.make_async_copy(own[i].at[v, :, :, side], own_buf[i].at[v], sems.at[place]))
            copies.append(pltpu.make_async_copy(got[i].at[v, :, :, side], got_buf[i].at[v], sems.at[place + 1]))
    for copy in copies:
        copy.start()
    for i, portion in enumerate(portions):
        for v in range(4):
            wait_all(copies[8 * i + 2 * v : 8 * i + 2 * v + 2])
            view = 4 * portion + v
            first, other = first_ref[view : view + 1], other_ref[view : view + 1]
            for b in range(PBLK):
                low, high = own_buf[i][v, 0], own_buf[i][v, 1]
                mine = jnp.where(first == b, low, jnp.where(first + 1 == b, high, 0.0))
                low, high = got_buf[i][v, 0], got_buf[i][v, 1]
                out[i][v, b] = mine + jnp.where(other == b, low, jnp.where(other + 1 == b, high, 0.0))


ANY = pl.BlockSpec(memory_space=pl.ANY)


def merge(first, other, crossing, portions, side):
    rows = crossing[0][0].shape[2] // 2
    cuts = [(1 << FIRST_BIT[w], rows >> FIRST_BIT[w]) for w in portions]
    count = len(portions)
    inputs = [crossing[w][k].reshape(4, 2, c[0], 2, c[1], PB) for k in range(2) for w, c in zip(portions, cuts)]
    buffers = [pltpu.VMEM((4, 2) + c + (PB,), jnp.float32) for c in cuts]
    return pl.pallas_call(
        functools.partial(merge_body, portions=portions, side=side),
        in_specs=[VMEM, VMEM] + [ANY] * (2 * count),
        out_specs=[VMEM] * count,
        out_shape=[pltpu.VMEM((4, PBLK) + c + (PB,), jnp.float32) for c in cuts],
        scratch_shapes=buffers * 2 + [pltpu.SemaphoreType.DMA((8 * count,))],
        cost_estimate=pl.CostEstimate(flops=count << 30, transcendentals=0, bytes_accessed=count << 21),
        compiler_params=vmem_params(3 * count + 1),
        name="merge_send" if side else "merge_keep",
    )(first, other, *inputs)


LARGEST = float(jnp.finfo(jnp.bfloat16).max)


def detect(natt_ref, resp_ref, row_of):
    high, low = [], []
    for v in range(16):
        power = natt_ref[0] * row_of(0, v)
        for m in range(1, MATS):
            power = power + natt_ref[m] * row_of(m, v)
        passed = jnp.exp(power)
        top = jnp.minimum(passed, LARGEST).astype(jnp.bfloat16)
        high.append(top)
        low.append((passed - top.astype(jnp.float32)).astype(jnp.bfloat16))
    terms = jnp.concatenate([jnp.concatenate(high, axis=1), jnp.concatenate(low, axis=1)], axis=0)
    got = jnp.dot(resp_ref[...], terms, preferred_element_type=jnp.float32)
    got = got[:CBINS] + got[CBINS:]
    return jnp.swapaxes(jnp.stack([got[:, v * PB : (v + 1) * PB] for v in range(16)]), 0, 1)


def split_response(response):
    top = lax.reduce_precision(response, 8, 7)
    rest = response - top
    rows = jnp.concatenate([jnp.concatenate([top, top], axis=1), jnp.pad(rest, ((0, 0), (0, EBINS)))], axis=0)
    return rows.astype(jnp.bfloat16)


DETECT_COST = pl.CostEstimate(flops=1 << 31, transcendentals=1 << 20, bytes_accessed=1 << 20)


def inner_body(cross_ref, near_share_ref, natt_ref, resp_ref, sums_ref, near_ref, partial_ref):
    def rows(ref, r, b):
        return lambda m, v: ref[m, r, PBLK * v + b : PBLK * v + b + 1, :]

    for b in range(PBLK):
        own = [detect(natt_ref, resp_ref, rows(sums_ref, r, b)) for r in (0, 1)]
        near = detect(natt_ref, resp_ref, rows(near_ref, 0, b))
        for c in range(CBINS):
            leak = cross_ref[c : c + 1]
            for row in (0, 1):
                share = near_share_ref[row, c : c + 1]
                side = jnp.where(share > 0.0, share * near[c], 0.0)
                partial_ref[c, row, b] = (1.0 - 2.0 * leak) * own[row][c] + leak * own[1 - row][c] + side


def inner(leak, share, natt, resp, sums, near):
    return pl.pallas_call(
        inner_body,
        in_specs=[VMEM] * 6,
        out_specs=VMEM,
        out_shape=jax.ShapeDtypeStruct((CBINS, 2, PBLK, 16, PB), jnp.float32),
        cost_estimate=DETECT_COST,
        compiler_params=vmem_params(8),
        name="inner",
    )(leak, share, natt, resp, sums, near)


def finish_body(far_share_ref, natt_ref, resp_ref, far_ref, partial_ref, out_ref):
    for b in range(PBLK):
        far = detect(natt_ref, resp_ref, lambda m, v: far_ref[m, 0, PBLK * v + b : PBLK * v + b + 1, :])
        for c in range(CBINS):
            for row in (0, 1):
                share = far_share_ref[row, c : c + 1]
                side = jnp.where(share > 0.0, share * far[c], 0.0)
                out_ref[c, row, :, b * PB : (b + 1) * PB] = partial_ref[c, row, b] + side


def finish(share, natt, resp, far, partial):
    return pl.pallas_call(
        finish_body,
        in_specs=[VMEM] * 5,
        out_specs=VMEM,
        out_shape=jax.ShapeDtypeStruct((CBINS, 2, 16, PBLK * PB), jnp.float32),
        cost_estimate=DETECT_COST,
        compiler_params=vmem_params(8),
        name="finish",
    )(share, natt, resp, far, partial)


def per_device(volume, system, geometry, attenuation, response, crosstalk):
    rows = volume.shape[1]
    depth = volume.shape[3]
    tile = lax.axis_index(TILE_AXES)
    vol = volume.reshape(rows, depth)
    matrix = system.reshape(depth, 32, PB)
    mine = lax.dynamic_index_in_dim(geometry, tile, 0, keepdims=False)
    partner = lax.dynamic_index_in_dim(geometry, tile ^ 1, 0, keepdims=False)
    mine, partner = (jnp.broadcast_to(t[:, None], (16, PB)) for t in (mine, partner))

    own, away, columns, *rest = project_first(vol, matrix)
    crossing = [None] * 4
    current = [None] * 4

    def cross(w, own, away):
        crossing[w] = own, lax.ppermute(away, "core", [(0, 1), (1, 0)])

    cross(0, own, away)
    others = project(columns, rest)
    for w in range(1, 4):
        cross(w, *others[w - 1])
    sends = []
    for group in SEND_GROUPS:
        sends += [part.astype(jnp.float16) for part in merge(mine, partner, crossing, group, 1)]
    crossing, sends[3] = lax.optimization_barrier((crossing, sends[3]))
    keeps = []
    for group in KEEP_GROUPS:
        keeps += merge(mine, partner, crossing, group, 0)
    for w in range(4):
        axis, which = ORDERS[w][0]
        shape = [4, PBLK, 2, 2, 2, 2, 16, PB]
        shape[2 + FIRST_BIT[w]] = 1
        got = lax.ppermute(sends[w], axis, PAIRS[which])
        current[w] = [keeps[w].reshape(shape), got.reshape(shape)]

    def total(parts):
        value = parts[0]
        for part in parts[1:]:
            value = value + part.astype(jnp.float32)
        return value

    for n in range(1, 4):
        sends = []
        for w in range(4):
            axis, which = ORDERS[w][n]
            dim = DIM_OF[axis, which]
            sent = total([lax.slice_in_dim(t, 1, 2, axis=dim) for t in current[w]]).astype(jnp.float16)
            current[w] = [lax.slice_in_dim(t, 0, 1, axis=dim) for t in current[w]]
            if n == 1:
                sent, kept = lax.optimization_barrier((sent, total(current[w])))
                current[w] = [kept]
            sends.append(sent)
        for w in range(4):
            axis, which = ORDERS[w][n]
            current[w].append(lax.ppermute(sends[w], axis, PAIRS[which]))
    for w in range(4):
        current[w] = total(current[w]).astype(jnp.float16)

    whole = jnp.concatenate([c.reshape(4, PBLK, MATS, 2, 2, PB) for c in current], axis=0)
    outgoing = whole.transpose(3, 2, 4, 0, 1, 5).reshape(8, 2, 64, PB)
    received = lax.all_to_all(outgoing, ("zh", "mat"), 0, 0, tiled=True)
    received = received.reshape(2, MATS, 2, 64, PB).astype(jnp.float32)
    sums = received[0] + received[1]

    core = lax.axis_index("core")
    rounded = sums.astype(jnp.float16)
    top, bottom = rounded[:, 0:1], rounded[:, 1:2]
    axes = ("mat",) + TILE_AXES
    count = lax.axis_size(axes)
    me = lax.axis_index(axes)
    swap = [(i, i + 1) for i in range(1, count - 1, 2)]
    near = lax.ppermute(jnp.where(core == 0, bottom, top), "core", [(0, 1), (1, 0)])
    far = lax.ppermute(jnp.where(core == 0, top, bottom), axes, swap + [(j, i) for i, j in swap])
    leak = jnp.broadcast_to(crosstalk[:, None], (CBINS, PB))
    present = jnp.logical_and(me > 0, me < count - 1)
    row = jnp.arange(2, dtype=jnp.int32)[:, None, None]
    near_share = jnp.where(row == 1 - core, leak, 0.0)
    far_share = jnp.where(jnp.logical_and(row == core, present), leak, 0.0)
    natt = jnp.broadcast_to(-attenuation[:, :, None], (MATS, EBINS, PB))
    resp = split_response(response)
    partial = inner(leak, near_share, natt, resp, sums, near.astype(jnp.float32))
    return finish(far_share, natt, resp, far.astype(jnp.float32), partial)


def solution(mesh):
    fine = Mesh(mesh.devices.reshape(4, 4, 2, 4, 2), AXES)
    in_specs = (P("mat", None, TILE_AXES, None), P(TILE_AXES, None, None, None), P(), P(), P(), P())
    out_specs = P(None, AXES, None, None)

    return jax.shard_map(per_device, mesh=fine, in_specs=in_specs, out_specs=out_specs, check_vma=False)
```

```python
import functools

import jax
import jax.numpy as jnp
from jax import lax
from jax.experimental import pallas as pl
from jax.experimental.pallas import tpu as pltpu
from jax.sharding import Mesh, PartitionSpec as P

PB = 128
PBLK = 4
CBINS = 8
EBINS = 64
MATS = 4
AXES = ("mat", "y", "zh", "x", "core")
TILE_AXES = ("y", "zh", "x", "core")
PAIRS = ([(0, 1), (1, 0), (2, 3), (3, 2)], [(1, 2), (2, 1), (3, 0), (0, 3)])
ORDERS = (
    (("x", 0), ("x", 1), ("y", 0), ("y", 1)),
    (("x", 1), ("x", 0), ("y", 1), ("y", 0)),
    (("y", 0), ("y", 1), ("x", 0), ("x", 1)),
    (("y", 1), ("y", 0), ("x", 1), ("x", 0)),
)
FIRST_BIT = (0, 1, 2, 3)
DIM_OF = {("x", 0): 2, ("x", 1): 3, ("y", 0): 4, ("y", 1): 5}


SEND_GROUPS = ((0,), (1,), (2,), (3,))
KEEP_GROUPS = ((0, 1, 2, 3),)


def pair_bits(i):
    return ((i + 1) >> 1) & 1, i >> 1


def row_order(slice_count):
    pos = lax.broadcasted_iota(jnp.int32, (slice_count, 1), 0)
    bits = [(pos >> (8 - n)) & 1 for n in range(5)]
    rest = pos & 15
    core = bits[0] ^ lax.axis_index("core")

    def place(b0, b1, name):
        mine = pair_bits(lax.axis_index(name))
        b0, b1 = b0 ^ mine[0], b1 ^ mine[1]
        return 2 * b1 + (b0 ^ b1)

    x = place(bits[1], bits[2], "x")
    y = place(bits[3], bits[4], "y")
    mat, zh, r = rest >> 2, (rest >> 1) & 1, rest & 1
    return mat * 128 + y * 32 + zh * 16 + x * 4 + core * 2 + r


def vmem_params(mib):
    return pltpu.CompilerParams(vmem_limit_bytes=mib << 20)


VMEM = pl.BlockSpec(memory_space=pltpu.VMEM)
SMEM = pl.BlockSpec(memory_space=pltpu.SMEM)
HBM = pl.BlockSpec(memory_space=pltpu.HBM)


def multiply(columns, matrix_ref, own_hbm, away_hbm, buf, sems):
    weights = jnp.swapaxes(matrix_ref[...], 0, 1)
    half = columns.shape[0] // 2
    copies = []
    for v in range(4):
        pair = jnp.concatenate([weights[2 * v], weights[2 * v + 1]], axis=1)
        got = jnp.dot(columns, pair, preferred_element_type=jnp.float32)
        buf[v, 0] = got[:, :PB]
        buf[v, 1] = got[:, PB:]
        copies.append(pltpu.make_async_copy(buf.at[v, :, pl.ds(half, half), :], away_hbm.at[v], sems.at[2 * v]))
        copies.append(pltpu.make_async_copy(buf.at[v, :, pl.ds(0, half), :], own_hbm.at[v], sems.at[2 * v + 1]))
        copies[-2].start()
        copies[-1].start()
    return copies


def wait_all(copies):
    for copy in copies:
        copy.wait()


def first_body(
    vol_hbm, sys_hbm, own_hbm, away_hbm, col_ref, m1_ref, m2_ref, m3_ref, vol_buf, m0_buf, buf, sems, out_sems
):
    copies = [pltpu.make_async_copy(vol_hbm, vol_buf, sems.at[4])]
    for w, target in enumerate((m0_buf, m1_ref, m2_ref, m3_ref)):
        copies.append(pltpu.make_async_copy(sys_hbm.at[:, pl.ds(8 * w, 8), :], target, sems.at[w]))
    for copy in copies:
        copy.start()
    rows = vol_buf.shape[0]
    chosen = (row_order(rows) == lax.broadcasted_iota(jnp.int32, (rows, rows), 1)).astype(jnp.bfloat16)
    copies[0].wait()
    columns = jnp.dot(chosen, vol_buf[...], preferred_element_type=jnp.float32).astype(jnp.bfloat16)
    col_ref[...] = columns
    copies[1].wait()
    outs = multiply(columns, m0_buf, own_hbm, away_hbm, buf, out_sems)
    wait_all(copies[2:])
    wait_all(outs)


def in_hbm(x):
    return pltpu.with_memory_space_constraint(x, pltpu.HBM)


def in_vmem(x):
    return pltpu.with_memory_space_constraint(x, pltpu.VMEM)


def project_first(vol, matrix):
    rows, depth = vol.shape
    half = pltpu.HBM((4, 2, rows // 2, PB), jnp.float32)
    part = pltpu.VMEM((depth, 8, PB), jnp.bfloat16)
    return pl.pallas_call(
        first_body,
        in_specs=[HBM, HBM],
        out_specs=[HBM] * 2 + [VMEM] * 4,
        out_shape=[half, half, pltpu.VMEM((rows, depth), jnp.bfloat16), part, part, part],
        scratch_shapes=[
            pltpu.VMEM((rows, depth), jnp.bfloat16),
            pltpu.VMEM((depth, 8, PB), jnp.bfloat16),
            pltpu.VMEM((4, 2, rows, PB), jnp.float32),
            pltpu.SemaphoreType.DMA((5,)),
            pltpu.SemaphoreType.DMA((8,)),
        ],
        cost_estimate=pl.CostEstimate(flops=2 * rows * depth * 12 * PB, transcendentals=0, bytes_accessed=12 << 20),
        compiler_params=vmem_params(16),
        name="project_first",
    )(in_hbm(vol), in_hbm(matrix))


def project_body(col_ref, *refs):
    matrices, outs, bufs, sems = refs[:3], refs[3:9], refs[9:12], refs[12:]
    columns = col_ref[...]
    copies = []
    for i in range(3):
        copies += multiply(columns, matrices[i], outs[2 * i], outs[2 * i + 1], bufs[i], sems[i])
    wait_all(copies)


def project(columns, matrices):
    rows, depth = columns.shape
    half = pltpu.HBM((4, 2, rows // 2, PB), jnp.float32)
    got = pl.pallas_call(
        project_body,
        in_specs=[VMEM] * 4,
        out_specs=[HBM] * 6,
        out_shape=[half] * 6,
        scratch_shapes=[pltpu.VMEM((4, 2, rows, PB), jnp.float32)] * 3 + [pltpu.SemaphoreType.DMA((8,))] * 3,
        cost_estimate=pl.CostEstimate(flops=6 * rows * depth * 8 * PB, transcendentals=0, bytes_accessed=15 << 20),
        compiler_params=vmem_params(14),
        name="project",
    )(in_vmem(columns), *[in_vmem(m) for m in matrices])
    return got[0:2], got[2:4], got[4:6]


def merge_body(first_ref, other_ref, *refs, portions, side):
    count = len(portions)
    own, got, out = refs[:count], refs[count : 2 * count], refs[2 * count : 3 * count]
    own_buf, got_buf, sems = refs[3 * count : 4 * count], refs[4 * count : 5 * count], refs[5 * count]
    copies = []
    for i in range(count):
        for v in range(4):
            place = 8 * i + 2 * v
            copies.append(pltpu.make_async_copy(own[i].at[v, :, :, side], own_buf[i].at[v], sems.at[place]))
            copies.append(pltpu.make_async_copy(got[i].at[v, :, :, side], got_buf[i].at[v], sems.at[place + 1]))
    for copy in copies:
        copy.start()
    for i, portion in enumerate(portions):
        for v in range(4):
            wait_all(copies[8 * i + 2 * v : 8 * i + 2 * v + 2])
            view = 4 * portion + v
            first, other = first_ref[view : view + 1], other_ref[view : view + 1]
            for b in range(PBLK):
                low, high = own_buf[i][v, 0], own_buf[i][v, 1]
                mine = jnp.where(first == b, low, jnp.where(first + 1 == b, high, 0.0))
                low, high = got_buf[i][v, 0], got_buf[i][v, 1]
                out[i][v, b] = mine + jnp.where(other == b, low, jnp.where(other + 1 == b, high, 0.0))


ANY = pl.BlockSpec(memory_space=pl.ANY)


def merge(first, other, crossing, portions, side):
    rows = crossing[0][0].shape[2] // 2
    cuts = [(1 << FIRST_BIT[w], rows >> FIRST_BIT[w]) for w in portions]
    count = len(portions)
    inputs = [crossing[w][k].reshape(4, 2, c[0], 2, c[1], PB) for k in range(2) for w, c in zip(portions, cuts)]
    buffers = [pltpu.VMEM((4, 2) + c + (PB,), jnp.float32) for c in cuts]
    return pl.pallas_call(
        functools.partial(merge_body, portions=portions, side=side),
        in_specs=[VMEM, VMEM] + [ANY] * (2 * count),
        out_specs=[VMEM] * count,
        out_shape=[pltpu.VMEM((4, PBLK) + c + (PB,), jnp.float32) for c in cuts],
        scratch_shapes=buffers * 2 + [pltpu.SemaphoreType.DMA((8 * count,))],
        cost_estimate=pl.CostEstimate(flops=count << 30, transcendentals=0, bytes_accessed=count << 21),
        compiler_params=vmem_params(3 * count + 1),
        name="merge_send" if side else "merge_keep",
    )(first, other, *inputs)


LARGEST = float(jnp.finfo(jnp.bfloat16).max)


def detect(natt_ref, resp_ref, row_of):
    high, low = [], []
    for v in range(16):
        power = natt_ref[0] * row_of(0, v)
        for m in range(1, MATS):
            power = power + natt_ref[m] * row_of(m, v)
        passed = jnp.exp(power)
        top = jnp.minimum(passed, LARGEST).astype(jnp.bfloat16)
        high.append(top)
        low.append((passed - top.astype(jnp.float32)).astype(jnp.bfloat16))
    terms = jnp.concatenate([jnp.concatenate(high, axis=1), jnp.concatenate(low, axis=1)], axis=0)
    got = jnp.dot(resp_ref[...], terms, preferred_element_type=jnp.float32)
    got = got[:CBINS] + got[CBINS:]
    return jnp.swapaxes(jnp.stack([got[:, v * PB : (v + 1) * PB] for v in range(16)]), 0, 1)


def split_response(response):
    top = lax.reduce_precision(response, 8, 7)
    rest = response - top
    rows = jnp.concatenate([jnp.concatenate([top, top], axis=1), jnp.pad(rest, ((0, 0), (0, EBINS)))], axis=0)
    return rows.astype(jnp.bfloat16)


DETECT_COST = pl.CostEstimate(flops=1 << 31, transcendentals=1 << 20, bytes_accessed=1 << 20)


def inner_body(cross_ref, near_share_ref, natt_ref, resp_ref, sums_ref, near_ref, partial_ref):
    def rows(ref, r, b):
        return lambda m, v: ref[m, r, PBLK * v + b : PBLK * v + b + 1, :]

    for b in range(PBLK):
        own = [detect(natt_ref, resp_ref, rows(sums_ref, r, b)) for r in (0, 1)]
        near = detect(natt_ref, resp_ref, rows(near_ref, 0, b))
        for c in range(CBINS):
            leak = cross_ref[c : c + 1]
            for row in (0, 1):
                share = near_share_ref[row, c : c + 1]
                side = jnp.where(share > 0.0, share * near[c], 0.0)
                partial_ref[c, row, b] = (1.0 - 2.0 * leak) * own[row][c] + leak * own[1 - row][c] + side


def inner(leak, share, natt, resp, sums, near):
    return pl.pallas_call(
        inner_body,
        in_specs=[VMEM] * 6,
        out_specs=VMEM,
        out_shape=jax.ShapeDtypeStruct((CBINS, 2, PBLK, 16, PB), jnp.float32),
        cost_estimate=DETECT_COST,
        compiler_params=vmem_params(8),
        name="inner",
    )(leak, share, natt, resp, sums, near)


def finish_body(far_share_ref, natt_ref, resp_ref, far_ref, partial_ref, out_hbm, out_ref, sems):
    copies = []
    for b in range(PBLK):
        far = detect(natt_ref, resp_ref, lambda m, v: far_ref[m, 0, PBLK * v + b : PBLK * v + b + 1, :])
        for c in range(CBINS):
            for row in (0, 1):
                share = far_share_ref[row, c : c + 1]
                side = jnp.where(share > 0.0, share * far[c], 0.0)
                out_ref[c, row, :, b * PB : (b + 1) * PB] = partial_ref[c, row, b] + side
        columns = (slice(None),) * 3 + (pl.ds(b * PB, PB),)
        copies.append(pltpu.make_async_copy(out_ref.at[columns], out_hbm.at[columns], sems.at[b]))
        copies[-1].start()
    wait_all(copies)


def finish(share, natt, resp, far, partial):
    return pl.pallas_call(
        finish_body,
        in_specs=[VMEM] * 5,
        out_specs=HBM,
        out_shape=pltpu.HBM((CBINS, 2, 16, PBLK * PB), jnp.float32),
        scratch_shapes=[pltpu.VMEM((CBINS, 2, 16, PBLK * PB), jnp.float32), pltpu.SemaphoreType.DMA((PBLK,))],
        cost_estimate=DETECT_COST,
        compiler_params=vmem_params(8),
        name="finish",
    )(share, natt, resp, far, partial)


def per_device(volume, system, geometry, attenuation, response, crosstalk):
    rows = volume.shape[1]
    depth = volume.shape[3]
    tile = lax.axis_index(TILE_AXES)
    vol = volume.reshape(rows, depth)
    matrix = system.reshape(depth, 32, PB)
    mine = lax.dynamic_index_in_dim(geometry, tile, 0, keepdims=False)
    partner = lax.dynamic_index_in_dim(geometry, tile ^ 1, 0, keepdims=False)
    mine, partner = (jnp.broadcast_to(t[:, None], (16, PB)) for t in (mine, partner))

    own, away, columns, *rest = project_first(vol, matrix)
    crossing = [None] * 4
    current = [None] * 4

    def cross(w, own, away):
        crossing[w] = own, lax.ppermute(away, "core", [(0, 1), (1, 0)])

    cross(0, own, away)
    others = project(columns, rest)
    for w in range(1, 4):
        cross(w, *others[w - 1])
    sends = []
    for group in SEND_GROUPS:
        sends += [part.astype(jnp.float16) for part in merge(mine, partner, crossing, group, 1)]
    crossing, sends[3] = lax.optimization_barrier((crossing, sends[3]))
    keeps = []
    for group in KEEP_GROUPS:
        keeps += merge(mine, partner, crossing, group, 0)
    for w in range(4):
        axis, which = ORDERS[w][0]
        shape = [4, PBLK, 2, 2, 2, 2, 16, PB]
        shape[2 + FIRST_BIT[w]] = 1
        got = lax.ppermute(sends[w], axis, PAIRS[which])
        current[w] = [keeps[w].reshape(shape), got.reshape(shape)]

    def total(parts):
        value = parts[0]
        for part in parts[1:]:
            value = value + part.astype(jnp.float32)
        return value

    for n in range(1, 4):
        sends = []
        for w in range(4):
            axis, which = ORDERS[w][n]
            dim = DIM_OF[axis, which]
            sent = total([lax.slice_in_dim(t, 1, 2, axis=dim) for t in current[w]]).astype(jnp.float16)
            current[w] = [lax.slice_in_dim(t, 0, 1, axis=dim) for t in current[w]]
            if n == 1:
                sent, kept = lax.optimization_barrier((sent, total(current[w])))
                current[w] = [kept]
            sends.append(sent)
        for w in range(4):
            axis, which = ORDERS[w][n]
            current[w].append(lax.ppermute(sends[w], axis, PAIRS[which]))
    for w in range(4):
        current[w] = total(current[w]).astype(jnp.float16)

    whole = jnp.concatenate([c.reshape(4, PBLK, MATS, 2, 2, PB) for c in current], axis=0)
    outgoing = whole.transpose(3, 2, 4, 0, 1, 5).reshape(8, 2, 64, PB)
    received = lax.all_to_all(outgoing, ("zh", "mat"), 0, 0, tiled=True)
    received = received.reshape(2, MATS, 2, 64, PB).astype(jnp.float32)
    sums = received[0] + received[1]

    core = lax.axis_index("core")
    rounded = sums.astype(jnp.float16)
    top, bottom = rounded[:, 0:1], rounded[:, 1:2]
    axes = ("mat",) + TILE_AXES
    count = lax.axis_size(axes)
    me = lax.axis_index(axes)
    swap = [(i, i + 1) for i in range(1, count - 1, 2)]
    near = lax.ppermute(jnp.where(core == 0, bottom, top), "core", [(0, 1), (1, 0)])
    far = lax.ppermute(jnp.where(core == 0, top, bottom), axes, swap + [(j, i) for i, j in swap])
    leak = jnp.broadcast_to(crosstalk[:, None], (CBINS, PB))
    present = jnp.logical_and(me > 0, me < count - 1)
    row = jnp.arange(2, dtype=jnp.int32)[:, None, None]
    near_share = jnp.where(row == 1 - core, leak, 0.0)
    far_share = jnp.where(jnp.logical_and(row == core, present), leak, 0.0)
    natt = jnp.broadcast_to(-attenuation[:, :, None], (MATS, EBINS, PB))
    resp = split_response(response)
    partial = inner(leak, near_share, natt, resp, sums, near.astype(jnp.float32))
    return finish(far_share, natt, resp, far.astype(jnp.float32), partial)


def solution(mesh):
    fine = Mesh(mesh.devices.reshape(4, 4, 2, 4, 2), AXES)
    in_specs = (P("mat", None, TILE_AXES, None), P(TILE_AXES, None, None, None), P(), P(), P(), P())
    out_specs = P(None, AXES, None, None)

    return jax.shard_map(per_device, mesh=fine, in_specs=in_specs, out_specs=out_specs, check_vma=False)
```
